32 devices in a mesh: groups: 2 (over y), seq: 4 (over z), tp: 4 (over x, core).
Axes of the slice: x: 2, y: 2, z: 4, core: 2. Of those that a mesh axis runs over, the one named last changes fastest.
Arguments:
- resp_queries: bfloat16 [4096, 8192], P(('groups', 'seq'), 'tp'), parts along dimension 0, may hold values from -300 to 300
- resp_keys: bfloat16 [4096, 1024], P(('groups', 'seq'), 'tp'), parts along dimension 0, may hold values from -4 to 4
- resp_values: bfloat16 [4096, 1024], P(('groups', 'seq'), 'tp'), parts along dimension 0, may hold values from -48 to 48
- prompt_keys: bfloat16 [2048, 1024], P(('groups', 'seq'), 'tp'), parts along dimension 0, may hold values from -4 to 4
- prompt_values: bfloat16 [2048, 1024], P(('groups', 'seq'), 'tp'), parts along dimension 0, may hold values from -48 to 48
- out_weight: bfloat16 [8192, 8192], P('tp', 'seq'), may hold values from -0.0625 to 0.0625
- resp_blocks: int32 [8], P('groups'), parts along dimension 0, may hold values from 1 to 4, 11 in all
Outputs:
- attended: bfloat16 [4096, 8192], P(('groups', 'seq'), 'tp'), parts along dimension 0
The draws below stay inside these ranges and needn't reach their ends.
There are 2 independent parts, one for each index of `groups`. The reference program is written for one: setup_inputs(seed, part) draws one part's arguments, and reference() takes and returns one part's arrays. A program takes and returns all parts, laid end to end along the dimension named above; an argument that names none is the same for every part. Nothing has to cross between parts.
Inputs may be any that keep to these rules, and one draw needn't show every extreme that they name: `resp_blocks`: the lengths sum to 11 blocks and the longest is exactly 4 blocks.
All inputs are finite; a program needn't handle non-finite values.
Results may differ from the reference program's by a relative error of at most 0.017.
Values may be sent and summed in bfloat16 or wider, within the bound.
A program may use at most 128 MiB of HBM per device.

```python
import math
import jax
import jax.numpy as jnp
import numpy as np
from jax import lax

D = 8192
H = 64
KVH = 8
HD = 128
BLOCK = 128
MAXB = 4
PROMPT = 1024
NRESP = 4
TOTB = 11
N_TP = 4


def prompt_base(key):
    base = jax.random.normal(jax.random.fold_in(key, 11), (PROMPT, KVH * HD), jnp.float32)
    base = jnp.clip(base, -4.0, 4.0)
    return base


def draw_prompt_keys(key, part):
    return prompt_base(key).astype(jnp.bfloat16)


def draw_resp_queries(key, part):
    count = NRESP * MAXB * BLOCK
    values = 1.5 * jax.random.normal(jax.random.fold_in(key, 23), (count, H * HD), jnp.float32)
    values = jnp.clip(values, -9.0, 9.0)
    return values.astype(jnp.bfloat16)


def block_scale(rng, dims, split, smallest, top_value):
    loudness, own = 1.0, jax.random.fold_in(rng, 6)
    for dim, shards_of in split:
        heights = jnp.exp(jax.random.uniform(jax.random.fold_in(own, dim), (shards_of,), jnp.float32, smallest / len(split), top_value / len(split)))
        loudness = loudness * jnp.repeat(heights, dims[dim] // shards_of).reshape([-1 if axis == dim else 1 for axis in range(len(dims))])
    return loudness


def length_profile(amount, total, limit, lean):
    loads = [(1 << 20) // math.isqrt(standing ** lean) + 1 for standing in range(2, amount + 1)]
    rest, given = total - limit - (amount - 1), [1] * (amount - 1)
    while rest > 0:
        candidates = [i for i in range(amount - 1) if given[i] < limit]
        pool, left = sum([loads[i] for i in candidates]), rest
        for i in candidates:
            extra = min(limit - given[i], max(1, left * loads[i] // pool), rest)
            given[i] = given[i] + extra
            rest = rest - extra
    return np.array([limit] + given)


def ragged_sizes(rng, number_of, total, reach, skew):
    if number_of == 2:
        one = jax.random.randint(rng, (), max(1, total - reach), min(reach, total - 1) + 1)
        return jnp.stack([one, total - one])
    lengths = jnp.asarray(length_profile(number_of, total, reach, skew), jnp.int32)
    twos = (number_of - 1) // 2
    source_of, receiver = lengths[1:1 + 2 * twos:2], lengths[2:2 + 2 * twos:2]
    slack = jnp.minimum(source_of - 1, reach - receiver)
    shifted = jax.random.randint(jax.random.fold_in(rng, 1), (twos,), 0, 1 << 20) % (slack + 1)
    lengths = lengths.at[1:1 + 2 * twos:2].set(source_of - shifted).at[2:2 + 2 * twos:2].set(receiver + shifted)
    return lengths[jax.random.permutation(jax.random.fold_in(rng, 2), number_of)]


def bell_draw(rng, shape, scale, bound, split=(), kind=jnp.bfloat16):
    loudness = block_scale(rng, shape, split, -0.22, 0.18) if split else 1.0
    drawn = jax.random.normal(rng, shape, jnp.float32) * scale * loudness
    return jnp.minimum(jnp.maximum(drawn, -bound), bound).astype(kind)


def setup_inputs(seed: int = 0, part: int = 0) -> dict:
    seeds = jax.random.split(jax.random.key(seed), 8)
    own_keys = jax.random.split(jax.random.fold_in(seeds[7], part), 8)
    return {
        "resp_queries": draw_resp_queries(jax.random.fold_in(jax.random.fold_in(seeds[7], part), 71), part),
        "resp_keys": bell_draw(own_keys[1], (NRESP * MAXB * BLOCK, KVH * HD), 1.0, 4.0, ((0, 4), (1, 4))),
        "resp_values": bell_draw(own_keys[2], (NRESP * MAXB * BLOCK, KVH * HD), 8.0, 48.0, ((0, 4), (1, 4))),
        "prompt_keys": draw_prompt_keys(jax.random.fold_in(jax.random.fold_in(seeds[7], part), 71), part),
        "prompt_values": bell_draw(own_keys[4], (PROMPT, KVH * HD), 8.0, 48.0, ((0, 4), (1, 4))),
        "out_weight": bell_draw(seeds[5], (H * HD, D), (H * HD) ** -0.5, 0.0625, ((0, 4), (1, 4))),
        "resp_blocks": ragged_sizes(own_keys[6], NRESP, TOTB, MAXB, 1).astype(jnp.int32),
    }


def reference(resp_queries, resp_keys, resp_values, prompt_keys, prompt_values, out_weight, resp_blocks):
    span = MAXB * BLOCK
    group = H // KVH
    scale = HD ** -0.5
    width = H * HD // N_TP
    prompt_k = prompt_keys.astype(jnp.float32)
    prompt_v = prompt_values.astype(jnp.float32)

    def one_response(packed):
        queries, keys, values, blocks = packed
        length = blocks * BLOCK
        position = jnp.arange(span, dtype=jnp.int32)
        all_keys = jnp.concatenate([prompt_k, keys.astype(jnp.float32)], axis=0)
        all_values = jnp.concatenate([prompt_v, values.astype(jnp.float32)], axis=0)
        allowed = jnp.concatenate([jnp.ones((span, PROMPT), dtype=bool), position[None, :] <= position[:, None]], axis=1)
        pieces = []
        for head_group in range(KVH):
            query_part = queries[:, head_group * group * HD:(head_group + 1) * group * HD].astype(jnp.float32).reshape(span, group, HD)
            key_part = all_keys[:, head_group * HD:(head_group + 1) * HD]
            value_part = all_values[:, head_group * HD:(head_group + 1) * HD]
            scores = jnp.einsum('qhd,nd->hqn', query_part, key_part) * scale
            scores = jnp.where(allowed[None], scores, -jnp.inf)
            top = jnp.max(scores, axis=-1, keepdims=True)
            expo = jnp.exp(scores - top)
            total = jnp.sum(expo, axis=-1, keepdims=True)
            rounded = lax.optimization_barrier(expo.astype(jnp.bfloat16)).astype(jnp.float32)
            numer = jnp.einsum('hqn,nd->hqd', rounded, value_part)
            heads = (numer / total).astype(jnp.bfloat16)
            pieces.append(jnp.transpose(heads, (1, 0, 2)).reshape(span, group * HD))
        attn = jnp.concatenate(pieces, axis=1)
        summed = jnp.zeros((span, D), jnp.float32)
        for tensor_index in range(N_TP):
            partial_value = jnp.dot(attn[:, tensor_index * width:(tensor_index + 1) * width], out_weight[tensor_index * width:(tensor_index + 1) * width], preferred_element_type=jnp.float32)
            summed = summed + lax.optimization_barrier(partial_value.astype(jnp.bfloat16)).astype(jnp.float32)
        live = position < length
        return jnp.where(live[:, None], summed, jnp.zeros_like(summed)).astype(jnp.bfloat16)

    result = lax.map(one_response, (resp_queries.reshape(NRESP, span, H * HD), resp_keys.reshape(NRESP, span, KVH * HD), resp_values.reshape(NRESP, span, KVH * HD), resp_blocks))
    return result.reshape(NRESP * span, D)
```

```python
import functools
import jax
import jax.numpy as jnp
from jax import lax
from jax.experimental import pallas as pl
from jax.experimental.pallas import tpu as pltpu
from jax.sharding import PartitionSpec as P

HD = 128
BLOCK = 128
MAXB = 4
LOG2E = 1.4426950408889634


def attend_block(q, kp, vp, kr, vr, first, rows):
    c = (HD ** -0.5) * LOG2E
    nt = (((1,), (1,)), ((), ()))
    sp = lax.dot_general(q, kp, nt, preferred_element_type=jnp.float32)
    sr = lax.dot_general(q, kr, nt, preferred_element_type=jnp.float32)
    qpos = lax.broadcasted_iota(jnp.int32, sr.shape, 0) % rows + first
    kpos = lax.broadcasted_iota(jnp.int32, sr.shape, 1)
    sr = jnp.where(kpos <= qpos, sr, -1e30)
    m = jnp.maximum(
        jnp.max(sp, axis=1, keepdims=True), jnp.max(sr, axis=1, keepdims=True)
    )
    ep = jnp.exp2((sp - m) * c)
    er = jnp.exp2((sr - m) * c)
    total = jnp.sum(ep, axis=1, keepdims=True) + jnp.sum(er, axis=1, keepdims=True)
    acc = jnp.dot(ep.astype(jnp.bfloat16), vp, preferred_element_type=jnp.float32)
    acc = acc + jnp.dot(er.astype(jnp.bfloat16), vr, preferred_element_type=jnp.float32)
    return (acc / total).astype(jnp.bfloat16)


MESH = pl.DeviceIdType.MESH
WPIECES = 4
NTILE = 512
SCORES = 1 << 20
MLAG_A = MAXB + 1
MLAG_C = MAXB + 5


def fused_kernel(
    nseq, ntp, group,
    lens_ref, q_ref, kr_ref, vr_ref, pk_ref, pv_ref, w_hbm, out_ref,
    pk_all, pv_all, w_ref, wm, ga, gb, part, half_in, quart_in, mig_in,
    p_send, p_recv, w_sem, wm_send, wm_recv, g_send, g_recv,
    a_send, a_recv, b_send, b_recv, f_send, f_recv, m_recv,
):
    s = lax.axis_index("seq")
    t = lax.axis_index("tp")
    core, x = lax.rem(t, 2), lax.div(t, 2)
    partner = t + 1 - 2 * core
    nx = ntp // 2
    per = nseq // ntp
    last = nseq - 1
    chunks = nseq * MAXB
    nmig = last * MAXB
    prows = pk_ref.shape[0]
    depth, cols = w_ref.shape
    mig = wm.shape[0]
    half = BLOCK // 2
    quart = half // nx
    my_quart = pl.ds(core * half + x * quart, quart)
    kv_local = kr_ref.shape[1] // HD
    has_right, has_left = s < last, s > 0
    is_end = (s == 0) | (s == last)
    is_pre = (s == 1) | (s == last - 1)
    end = jnp.where(s < nseq // 2, 0, last)
    inward = jnp.where(s < nseq // 2, 1, -1)

    def p_copy(r, side, kv, own=False):
        dst = (pk_all, pv_all)[kv]
        src = (pk_ref, pv_ref)[kv] if own else dst.at[pl.ds(r * prows, prows)]
        return pltpu.make_async_remote_copy(
            src_ref=src,
            dst_ref=dst.at[pl.ds(r * prows, prows)],
            send_sem=p_send.at[side, r, kv],
            recv_sem=p_recv.at[r, kv],
            device_id={"seq": s - 1 + 2 * side},
            device_id_type=MESH,
        )

    def w_local(k):
        rows = pl.ds(k * (depth // WPIECES), depth // WPIECES)
        return pltpu.make_async_copy(w_hbm.at[rows], w_ref.at[rows], w_sem.at[k])

    def w_copy(k):
        rows = pl.ds(k * (mig // WPIECES), mig // WPIECES)
        return pltpu.make_async_remote_copy(
            src_ref=w_hbm.at[rows],
            dst_ref=wm.at[rows],
            send_sem=wm_send.at[k],
            recv_sem=wm_recv.at[k],
            device_id={"seq": jnp.where(is_end, s + inward, end)},
            device_id_type=MESH,
        )

    def g_copy(h, r, b, side):
        buf = (ga, gb)[h]
        return pltpu.make_async_remote_copy(
            src_ref=buf.at[r, b],
            dst_ref=buf.at[r, b],
            send_sem=g_send.at[h, side, r, b],
            recv_sem=g_recv.at[h, r, b],
            device_id={"seq": s - 1 + 2 * side},
            device_id_type=MESH,
        )

    def a_copy(i):
        return pltpu.make_async_remote_copy(
            src_ref=part.at[i, pl.ds((1 - core) * half, half)],
            dst_ref=half_in.at[i],
            send_sem=a_send.at[i],
            recv_sem=a_recv.at[i],
            device_id={"tp": partner},
            device_id_type=MESH,
        )

    def b_copy(i, k):
        other = lax.rem(x + k, nx)
        return pltpu.make_async_remote_copy(
            src_ref=part.at[i, pl.ds(core * half + other * quart, quart)],
            dst_ref=quart_in.at[i, k - 1],
            send_sem=b_send.at[i, k - 1],
            recv_sem=b_recv.at[i, k - 1],
            device_id={"tp": other * 2 + core},
            device_id_type=MESH,
        )

    def row_of(b):
        return b * BLOCK + core * half + x * quart

    def f_copy(i, r, b, owner):
        home, slab = lax.div(owner, per), lax.rem(owner, per)
        return pltpu.make_async_remote_copy(
            src_ref=part.at[i, my_quart],
            dst_ref=out_ref.at[slab, pl.ds(row_of(b), quart)],
            send_sem=f_send.at[i],
            recv_sem=f_recv.at[b, slab, t],
            device_id={"seq": r, "tp": home},
            device_id_type=MESH,
        )

    def m_copy(i, m):
        return pltpu.make_async_remote_copy(
            src_ref=part.at[i, my_quart],
            dst_ref=mig_in.at[m],
            send_sem=f_send.at[i],
            recv_sem=m_recv.at[m],
            device_id={"seq": jnp.where(is_end, s + inward, end)},
            device_id_type=MESH,
        )

    both = jnp.minimum(s, last - s)
    far_side = jnp.where(s > last - s, -1, 1)

    def chunk_of(i):
        j = jnp.maximum(i - MAXB, 0)
        twin = 2 * MAXB
        jj = jnp.maximum(j - twin * both, 0)
        near = j < twin * both
        d = jnp.where(near, lax.div(j, twin) + 1, both + 1 + lax.div(jj, MAXB))
        b = jnp.where(near, lax.div(lax.rem(j, twin), 2), lax.rem(jj, MAXB))
        side = jnp.where(near, 2 * lax.rem(j, 2) - 1, far_side)
        own = i < MAXB
        return jnp.where(own, s, s + side * d), jnp.where(own, i, b)

    def mig_of(m):
        return end + inward * (1 + lax.div(m, MAXB)), lax.rem(m, MAXB)

    def loop(n, fn, start=0):
        def step(i, carry):
            fn(i)
            return carry

        lax.fori_loop(start, n, step, 0)

    def goes(h, r, side):
        if side:
            ok = has_right & (r <= s)
            return ok & (s + 1 < last) if h == 0 else ok
        ok = has_left & (r >= s)
        return ok & (s > 1) if h == 0 else ok

    def send(h, r, b):
        for side in (1, 0):
            @pl.when(goes(h, r, side))
            def _():
                g_copy(h, r, b, side).start()

    for side, ok in ((0, has_left), (1, has_right)):
        @pl.when(ok)
        def _():
            p_copy(s, side, 0, own=True).start()
            p_copy(s, side, 1, own=True).start()

    @pl.when(is_end)
    def _():
        for k in range(WPIECES):
            w_copy(k).start()

    for k in range(WPIECES):
        w_local(k).start()

    pk_all[pl.ds(s * prows, prows), :] = pk_ref[...]
    pv_all[pl.ds(s * prows, prows), :] = pv_ref[...]

    def gather_prompt(d):
        for ok, r, side, onward in (
            (s - d >= 0, s - d, 1, has_right),
            (s + d < nseq, s + d, 0, has_left),
        ):
            @pl.when(ok)
            def _():
                for kv in range(2):
                    p_copy(r, side, kv).wait_recv()

                    @pl.when(onward)
                    def _():
                        p_copy(r, side, kv).start()

    loop(nseq, gather_prompt, 1)

    def project(i, r, b, full):
        @pl.when(full)
        def _():
            def tile(j):
                c = pl.ds(pl.multiple_of(j * NTILE, NTILE), NTILE)
                y = jnp.dot(ga[r, b], w_ref[:mig, c], preferred_element_type=jnp.float32)
                y = y + jnp.dot(gb[r, b], w_ref[mig:, c], preferred_element_type=jnp.float32)
                part[i, :, c] = y.astype(jnp.bfloat16)

            loop(cols // NTILE, tile)

        @pl.when(jnp.logical_not(full))
        def _():
            def tile(j):
                c = pl.ds(pl.multiple_of(j * NTILE, NTILE), NTILE)
                y = jnp.dot(gb[r, b], w_ref[mig:, c], preferred_element_type=jnp.float32)
                part[i, :, c] = y.astype(jnp.bfloat16)

            loop(cols // NTILE, tile)

        a_copy(i).start()

    def stage_a(i):
        r, b = chunk_of(i)

        @pl.when(i < MAXB)
        def _():
            first = i * BLOCK
            run = max(group // 2, 1)
            while run % 2 == 0 and run * BLOCK * pk_all.shape[0] > SCORES:
                run //= 2
            sent = False
            for k in range(kv_local):
                kvc = slice(k * HD, (k + 1) * HD)
                for h in range(k * group, (k + 1) * group, run):
                    q = jnp.concatenate(
                        [
                            q_ref[pl.ds(first, BLOCK), (h + g) * HD : (h + g + 1) * HD]
                            for g in range(run)
                        ],
                        axis=0,
                    )
                    o = attend_block(
                        q, pk_all[:, kvc], pv_all[:, kvc], kr_ref[:, kvc], vr_ref[:, kvc],
                        first, BLOCK,
                    )
                    for g in range(run):
                        at = (h + g) * HD
                        y = o[g * BLOCK : (g + 1) * BLOCK]
                        if at < mig:
                            ga[s, i, :, at : at + HD] = y
                        else:
                            gb[s, i, :, at - mig : at - mig + HD] = y
                    if not sent and (h + run) * HD >= mig:
                        sent = True
                        send(0, s, i)
            send(1, s, i)

        @pl.when(i >= MAXB)
        def _():
            @pl.when(jnp.logical_not(is_end))
            def _():
                g_copy(0, r, b, 0).wait_recv()

            send(0, r, b)
            g_copy(1, r, b, 0).wait_recv()
            send(1, r, b)

        @pl.when(i == 0)
        def _():
            for k in range(WPIECES):
                w_local(k).wait()

        project(i, r, b, (i < MAXB) | jnp.logical_not(is_end))

    def stage_b(i):
        a_copy(i).wait_recv()
        mine = pl.ds(core * half, half)
        part[i, mine, :] = (
            part[i, mine, :].astype(jnp.float32) + half_in[i].astype(jnp.float32)
        ).astype(jnp.bfloat16)
        for k in range(1, nx):
            b_copy(i, k).start()

    def reduced(i):
        for k in range(1, nx):
            b_copy(i, k).wait_recv()
        total = part[i, my_quart, :].astype(jnp.float32)
        for k in range(1, nx):
            total = total + quart_in[i, k - 1].astype(jnp.float32)
        return total

    def live(total, r, b):
        row = lax.broadcasted_iota(jnp.int32, total.shape, 0) + row_of(b)
        return jnp.where(row < lens_ref[r] * BLOCK, total, 0.0).astype(jnp.bfloat16)

    def stays(r, owner):
        return (r == s) & (lax.div(owner, per) == t)

    def deliver(i, r, b, owner):
        here = stays(r, owner)

        @pl.when(here)
        def _():
            out_ref[lax.rem(owner, per), pl.ds(row_of(b), quart), :] = part[i, my_quart, :]

        @pl.when(jnp.logical_not(here))
        def _():
            f_copy(i, r, b, owner).start()

    def hands_over(r):
        return is_end & (r != s)

    def stage_c(i):
        r, b = chunk_of(i)
        total = reduced(i)

        @pl.when(hands_over(r))
        def _():
            part[i, my_quart, :] = total.astype(jnp.bfloat16)
            m_copy(i, i - MAXB).start()

        @pl.when(jnp.logical_not(hands_over(r)))
        def _():
            part[i, my_quart, :] = live(total, r, b)
            deliver(i, r, b, s)

    def mig_a(m):
        r, b = mig_of(m)
        i = chunks + m

        @pl.when(m == 0)
        def _():
            for k in range(WPIECES):
                w_copy(k).wait_recv()

        def tile(j):
            c = pl.ds(pl.multiple_of(j * NTILE, NTILE), NTILE)
            y = jnp.dot(ga[r, b], wm[:, c], preferred_element_type=jnp.float32)
            part[i, :, c] = y.astype(jnp.bfloat16)

        loop(cols // NTILE, tile)
        a_copy(i).start()

    def mig_c(m):
        r, b = mig_of(m)
        i = chunks + m
        total = reduced(i)
        m_copy(i, m).wait_recv()
        part[i, my_quart, :] = live(total + mig_in[m].astype(jnp.float32), r, b)
        deliver(i, r, b, end)

    def step(i):
        @pl.when(i < chunks)
        def _():
            stage_a(i)

        @pl.when((i >= 1) & (i < chunks + 1))
        def _():
            stage_b(i - 1)

        @pl.when((i >= 2) & (i < chunks + 2))
        def _():
            stage_c(i - 2)

        @pl.when(is_pre & (i >= MLAG_A) & (i < MLAG_A + nmig))
        def _():
            mig_a(i - MLAG_A)

        @pl.when(is_pre & (i >= MLAG_A + 1) & (i < MLAG_A + 1 + nmig))
        def _():
            stage_b(chunks + i - MLAG_A - 1)

        @pl.when(is_pre & (i >= MLAG_C) & (i < MLAG_C + nmig))
        def _():
            mig_c(i - MLAG_C)

    loop(max(chunks + 2, MLAG_C + nmig), step)

    def drain_send(i):
        r, b = chunk_of(i)
        for h in range(2):
            for side in (1, 0):
                @pl.when(goes(h, r, side) & ((r == s) | jnp.logical_not(is_end)))
                def _():
                    g_copy(h, r, b, side).wait_send()

        a_copy(i).wait_send()
        for k in range(1, nx):
            b_copy(i, k).wait_send()

        @pl.when(hands_over(r))
        def _():
            m_copy(i, i - MAXB).wait_send()

        @pl.when(jnp.logical_not(hands_over(r) | stays(r, s)))
        def _():
            f_copy(i, r, b, s).wait_send()

    loop(chunks, drain_send)

    @pl.when(is_pre)
    def _():
        def drain_mig(m):
            r, b = mig_of(m)
            i = chunks + m
            a_copy(i).wait_send()
            for k in range(1, nx):
                b_copy(i, k).wait_send()

            @pl.when(jnp.logical_not(stays(r, end)))
            def _():
                f_copy(i, r, b, end).wait_send()

        loop(nmig, drain_mig)

    @pl.when(is_end)
    def _():
        for k in range(WPIECES):
            w_copy(k).wait_send()

    def drain_prompt(r):
        for kv in range(2):
            @pl.when(has_right & (r <= s))
            def _():
                p_copy(r, 1, kv).wait_send()

            @pl.when(has_left & (r >= s))
            def _():
                p_copy(r, 0, kv).wait_send()

    loop(nseq, drain_prompt)

    def drain_out(m):
        b = lax.div(m, per * ntp)
        j = lax.div(lax.rem(m, per * ntp), ntp)
        u = lax.rem(m, ntp)
        owner = t * per + j
        far = owner != s
        origin = jnp.where(far & (owner == 0), 1, jnp.where(far & (owner == last), last - 1, owner))

        @pl.when(jnp.logical_not((origin == s) & (u == t)))
        def _():
            row = b * BLOCK + lax.rem(u, 2) * half + lax.div(u, 2) * quart
            pltpu.make_async_remote_copy(
                src_ref=part.at[0, my_quart],
                dst_ref=out_ref.at[j, pl.ds(row, quart)],
                send_sem=f_send.at[0],
                recv_sem=f_recv.at[b, j, u],
                device_id={"seq": s, "tp": partner},
                device_id_type=MESH,
            ).wait_recv()

    loop(MAXB * per * ntp, drain_out)


def per_device(
    resp_queries, resp_keys, resp_values, prompt_keys, prompt_values, out_weight, resp_blocks
):
    nseq = lax.axis_size("seq")
    ntp = lax.axis_size("tp")
    rows, depth = resp_queries.shape
    assert rows == MAXB * BLOCK and nseq % ntp == 0 and ntp % 2 == 0 and nseq >= 4
    nx, per, chunks = ntp // 2, nseq // ntp, nseq * MAXB
    nmig = (nseq - 1) * MAXB
    every = chunks + nmig
    cols = out_weight.shape[1]
    mig = depth // HD // 4 * HD
    prows, kvw = prompt_keys.shape
    quart = BLOCK // ntp
    bf = jnp.bfloat16
    dma = pltpu.SemaphoreType.DMA
    vmem = pl.BlockSpec(memory_space=pltpu.VMEM)
    out = pl.pallas_call(
        functools.partial(fused_kernel, nseq, ntp, depth // resp_keys.shape[1]),
        out_shape=jax.ShapeDtypeStruct((per, rows, cols), bf),
        in_specs=[pl.BlockSpec(memory_space=pltpu.SMEM)]
        + [vmem] * 5
        + [pl.BlockSpec(memory_space=pl.ANY)],
        out_specs=vmem,
        scratch_shapes=[
            pltpu.VMEM((nseq * prows, kvw), bf),
            pltpu.VMEM((nseq * prows, kvw), bf),
            pltpu.VMEM((depth, cols), bf),
            pltpu.VMEM((mig, cols), bf),
            pltpu.VMEM((nseq, MAXB, BLOCK, mig), bf),
            pltpu.VMEM((nseq, MAXB, BLOCK, depth - mig), bf),
            pltpu.VMEM((every, BLOCK, cols), bf),
            pltpu.VMEM((every, BLOCK // 2, cols), bf),
            pltpu.VMEM((every, max(nx - 1, 1), quart, cols), bf),
            pltpu.VMEM((nmig, quart, cols), bf),
            dma((2, nseq, 2)),
            dma((nseq, 2)),
            dma((WPIECES,)),
            dma((WPIECES,)),
            dma((WPIECES,)),
            dma((2, 2, nseq, MAXB)),
            dma((2, nseq, MAXB)),
            dma((every,)),
            dma((every,)),
            dma((every, max(nx - 1, 1))),
            dma((every, max(nx - 1, 1))),
            dma((every,)),
            dma((MAXB, per, ntp)),
            dma((nmig,)),
        ],
        compiler_params=pltpu.CompilerParams(
            has_side_effects=True, vmem_limit_bytes=61000 * 1024
        ),
    )(resp_blocks, resp_queries, resp_keys, resp_values, prompt_keys, prompt_values, out_weight)
    return out.transpose(1, 0, 2).reshape(rows, per * cols)


def solution(mesh):
    return jax.shard_map(
        per_device,
        mesh=mesh,
        in_specs=(
            P(("groups", "seq"), "tp"),
            P(("groups", "seq"), "tp"),
            P(("groups", "seq"), "tp"),
            P(("groups", "seq"), "tp"),
            P(("groups", "seq"), "tp"),
            P("tp", "seq"),
            P("groups"),
        ),
        out_specs=P(("groups", "seq"), "tp"),
        check_vma=False,
    )
```

```python
import functools
import jax
import jax.numpy as jnp
from jax import lax
from jax.experimental import pallas as pl
from jax.experimental.pallas import tpu as pltpu
from jax.sharding import PartitionSpec as P

HD = 128
BLOCK = 128
MAXB = 4
LOG2E = 1.4426950408889634


def scores(q, kp, kr):
    nt = (((1,), (1,)), ((), ()))
    sp = lax.dot_general(q, kp, nt, preferred_element_type=jnp.float32)
    sr = lax.dot_general(q, kr, nt, preferred_element_type=jnp.float32)
    return sp, sr


def attend(sp, sr, vp, vr, first, rows):
    c = (HD ** -0.5) * LOG2E
    qpos = lax.broadcasted_iota(jnp.int32, sr.shape, 0) % rows + first
    kpos = lax.broadcasted_iota(jnp.int32, sr.shape, 1)
    sr = jnp.where(kpos <= qpos, sr, -1e30)
    m = jnp.maximum(
        jnp.max(sp, axis=1, keepdims=True), jnp.max(sr, axis=1, keepdims=True)
    )
    ep = jnp.exp2((sp - m) * c)
    er = jnp.exp2((sr - m) * c)
    total = jnp.sum(ep, axis=1, keepdims=True) + jnp.sum(er, axis=1, keepdims=True)
    acc = jnp.dot(ep.astype(jnp.bfloat16), vp, preferred_element_type=jnp.float32)
    acc = acc + jnp.dot(er.astype(jnp.bfloat16), vr, preferred_element_type=jnp.float32)
    return (acc / total).astype(jnp.bfloat16)


MESH = pl.DeviceIdType.MESH
WPIECES = 4
PIECES = 4
ORDER = (1, 2, 3, 0)
NTILE = 512
SCORES = 3 << 18
LAG_B = 1
LAG_C = 3
MLAG_A = MAXB + 1
LATE = 2


def fused_kernel(
    nseq, ntp, group,
    lens_ref, q_ref, kr_ref, vr_ref, pk_ref, pv_ref, w_hbm, out_ref,
    pk_all, pv_all, w_ref, wm, gath, part, half_in, quart_in, mig_in,
    p_send, p_recv, w_sem, wm_send, wm_recv, g_send, g_recv,
    a_send, a_recv, b_send, b_recv, f_send, f_recv, m_recv,
):
    s = lax.axis_index("seq")
    t = lax.axis_index("tp")
    core, x = lax.rem(t, 2), lax.div(t, 2)
    partner = t + 1 - 2 * core
    nx = ntp // 2
    per = nseq // ntp
    last = nseq - 1
    chunks = nseq * MAXB
    nmig = last * MAXB
    prows = pk_ref.shape[0]
    depth, cols = w_ref.shape
    mig = wm.shape[0]
    half = BLOCK // 2
    quart = half // nx
    my_quart = pl.ds(core * half + x * quart, quart)
    kv_local = kr_ref.shape[1] // HD
    has_right, has_left = s < last, s > 0
    is_end = (s == 0) | (s == last)
    is_pre = (s == 1) | (s == last - 1)
    end = jnp.where(s < nseq // 2, 0, last)
    inward = jnp.where(s < nseq // 2, 1, -1)

    def p_copy(r, side, kv, own=False):
        dst = (pk_all, pv_all)[kv]
        src = (pk_ref, pv_ref)[kv] if own else dst.at[pl.ds(r * prows, prows)]
        return pltpu.make_async_remote_copy(
            src_ref=src,
            dst_ref=dst.at[pl.ds(r * prows, prows)],
            send_sem=p_send.at[side, r, kv],
            recv_sem=p_recv.at[r, kv],
            device_id={"seq": s - 1 + 2 * side},
            device_id_type=MESH,
        )

    def w_local(k):
        rows = pl.ds(k * (depth // WPIECES), depth // WPIECES)
        return pltpu.make_async_copy(w_hbm.at[rows], w_ref.at[rows], w_sem.at[k])

    def w_copy(k):
        rows = pl.ds(k * (mig // WPIECES), mig // WPIECES)
        return pltpu.make_async_remote_copy(
            src_ref=w_hbm.at[rows],
            dst_ref=wm.at[rows],
            send_sem=wm_send.at[k],
            recv_sem=wm_recv.at[k],
            device_id={"seq": jnp.where(is_end, s + inward, end)},
            device_id_type=MESH,
        )

    def g_copy(h, r, b, side):
        return pltpu.make_async_remote_copy(
            src_ref=gath.at[r, b, h],
            dst_ref=gath.at[r, b, h],
            send_sem=g_send.at[h, side, r, b],
            recv_sem=g_recv.at[h, r, b],
            device_id={"seq": s - 1 + 2 * side},
            device_id_type=MESH,
        )

    def a_copy(i):
        return pltpu.make_async_remote_copy(
            src_ref=part.at[i, pl.ds((1 - core) * half, half)],
            dst_ref=half_in.at[i],
            send_sem=a_send.at[i],
            recv_sem=a_recv.at[i],
            device_id={"tp": partner},
            device_id_type=MESH,
        )

    def b_copy(i, k):
        other = lax.rem(x + k, nx)
        return pltpu.make_async_remote_copy(
            src_ref=part.at[i, pl.ds(core * half + other * quart, quart)],
            dst_ref=quart_in.at[i, k - 1],
            send_sem=b_send.at[i, k - 1],
            recv_sem=b_recv.at[i, k - 1],
            device_id={"tp": other * 2 + core},
            device_id_type=MESH,
        )

    def row_of(b):
        return b * BLOCK + core * half + x * quart

    def f_copy(i, r, b, owner):
        home, slab = lax.div(owner, per), lax.rem(owner, per)
        return pltpu.make_async_remote_copy(
            src_ref=part.at[i, my_quart],
            dst_ref=out_ref.at[slab, pl.ds(row_of(b), quart)],
            send_sem=f_send.at[i],
            recv_sem=f_recv.at[b, slab, t],
            device_id={"seq": r, "tp": home},
            device_id_type=MESH,
        )

    def m_copy(i, m):
        return pltpu.make_async_remote_copy(
            src_ref=part.at[i, my_quart],
            dst_ref=mig_in.at[m],
            send_sem=f_send.at[i],
            recv_sem=m_recv.at[m],
            device_id={"seq": jnp.where(is_end, s + inward, end)},
            device_id_type=MESH,
        )

    both = jnp.minimum(s, last - s)
    far_side = jnp.where(s > last - s, -1, 1)

    def chunk_of(i):
        j = jnp.maximum(i - MAXB, 0)
        twin = 2 * MAXB
        jj = jnp.maximum(j - twin * both, 0)
        near = j < twin * both
        d = jnp.where(near, lax.div(j, twin) + 1, both + 1 + lax.div(jj, MAXB))
        b = jnp.where(near, lax.div(lax.rem(j, twin), 2), lax.rem(jj, MAXB))
        side = jnp.where(near, 2 * lax.rem(j, 2) - 1, far_side)
        before = jnp.clip(lax.div(j - 2, 2), 0, MAXB)
        outer = (j >= 3) & (j < 3 + twin) & (lax.rem(j, 2) == 1)
        inner = j - before
        side = jnp.where(is_pre, jnp.where(outer, -inward, inward), side)
        d = jnp.where(is_pre, jnp.where(outer, 1, 1 + lax.div(inner, MAXB)), d)
        b = jnp.where(is_pre, jnp.where(outer, before, lax.rem(inner, MAXB)), b)
        own = i < MAXB
        return jnp.where(own, s, s + side * d), jnp.where(own, i, b)

    def mig_of(m):
        return end + inward * (1 + lax.div(m, MAXB)), lax.rem(m, MAXB)

    def loop(n, fn, start=0):
        def step(i, carry):
            fn(i)
            return carry

        lax.fori_loop(start, n, step, 0)

    def goes(h, r, side):
        if side:
            ok = has_right & (r <= s)
            return ok & (s + 1 < last) if h == 0 else ok
        ok = has_left & (r >= s)
        return ok & (s > 1) if h == 0 else ok

    def send(h, r, b):
        for side in (1, 0):
            @pl.when(goes(h, r, side))
            def _():
                g_copy(h, r, b, side).start()

    for side, ok in ((0, has_left), (1, has_right)):
        @pl.when(ok)
        def _():
            p_copy(s, side, 0, own=True).start()
            p_copy(s, side, 1, own=True).start()

    @pl.when(is_end)
    def _():
        for k in range(WPIECES):
            w_copy(k).start()

    for k in range(WPIECES):
        w_local(k).start()

    pk_all[pl.ds(s * prows, prows), :] = pk_ref[...]
    pv_all[pl.ds(s * prows, prows), :] = pv_ref[...]

    def gather_prompt(d):
        for ok, r, side, onward in (
            (s - d >= 0, s - d, 1, has_right),
            (s + d < nseq, s + d, 0, has_left),
        ):
            @pl.when(ok)
            def _():
                for kv in range(2):
                    p_copy(r, side, kv).wait_recv()

                    @pl.when(onward)
                    def _():
                        p_copy(r, side, kv).start()

    loop(nseq, gather_prompt, 1)

    def times(r, b, c, pieces):
        y = 0.0
        for h in pieces:
            y = y + jnp.dot(
                gath[r, b, h], w_ref[h * mig : (h + 1) * mig, c], preferred_element_type=jnp.float32
            )
        return y.astype(jnp.bfloat16)

    def project(i, r, b, full):
        for ok, pieces in ((full, range(PIECES)), (jnp.logical_not(full), range(1, PIECES))):
            @pl.when(ok)
            def _():
                def tile(j):
                    c = pl.ds(pl.multiple_of(j * NTILE, NTILE), NTILE)
                    part[i, :, c] = times(r, b, c, pieces)

                loop(cols // NTILE, tile)

        a_copy(i).start()

    def stage_a(i):
        r, b = chunk_of(i)

        @pl.when(i < MAXB)
        def _():
            first = i * BLOCK
            heads = mig // HD
            run = min(max(group // 2, 1), heads)
            while run % 2 == 0 and run * BLOCK * pk_all.shape[0] > SCORES:
                run //= 2
            runs = [h for p in ORDER for h in range(p * heads, (p + 1) * heads, run)]

            def kv_cols(h):
                return slice(h // group * HD, (h // group + 1) * HD)

            def score(h):
                q = jnp.concatenate(
                    [
                        q_ref[pl.ds(first, BLOCK), (h + g) * HD : (h + g + 1) * HD]
                        for g in range(run)
                    ],
                    axis=0,
                )
                return scores(q, pk_all[:, kv_cols(h)], kr_ref[:, kv_cols(h)])

            ready = score(runs[0])
            for n, h in enumerate(runs):
                now = ready
                if n + 1 < len(runs):
                    ready = score(runs[n + 1])
                o = attend(*now, pv_all[:, kv_cols(h)], vr_ref[:, kv_cols(h)], first, BLOCK)
                p = h // heads
                for g in range(run):
                    at = (h + g - p * heads) * HD
                    gath[s, i, p, :, at : at + HD] = o[g * BLOCK : (g + 1) * BLOCK]
                if h + run == (p + 1) * heads:
                    send(p, s, i)

        @pl.when(i >= MAXB)
        def _():
            for p in ORDER:
                @pl.when(jnp.logical_not(is_end) | (p > 0))
                def _():
                    g_copy(p, r, b, 0).wait_recv()

                send(p, r, b)

        @pl.when(i == 0)
        def _():
            for k in range(WPIECES):
                w_local(k).wait()

        project(i, r, b, (i < MAXB) | jnp.logical_not(is_end))

    def stage_b(i):
        a_copy(i).wait_recv()
        mine = pl.ds(core * half, half)
        part[i, mine, :] = (
            part[i, mine, :].astype(jnp.float32) + half_in[i].astype(jnp.float32)
        ).astype(jnp.bfloat16)
        for k in range(1, nx):
            b_copy(i, k).start()

    def reduced(i):
        for k in range(1, nx):
            b_copy(i, k).wait_recv()
        total = part[i, my_quart, :].astype(jnp.float32)
        for k in range(1, nx):
            total = total + quart_in[i, k - 1].astype(jnp.float32)
        return total

    def live(total, r, b):
        row = lax.broadcasted_iota(jnp.int32, total.shape, 0) + row_of(b)
        return jnp.where(row < lens_ref[r] * BLOCK, total, 0.0).astype(jnp.bfloat16)

    def stays(r, owner):
        return (r == s) & (lax.div(owner, per) == t)

    def deliver(i, r, b, owner):
        here = stays(r, owner)

        @pl.when(here)
        def _():
            out_ref[lax.rem(owner, per), pl.ds(row_of(b), quart), :] = part[i, my_quart, :]

        @pl.when(jnp.logical_not(here))
        def _():
            f_copy(i, r, b, owner).start()

    def hands_over(r):
        return is_end & (r != s)

    def stage_c(i):
        r, b = chunk_of(i)
        total = reduced(i)

        @pl.when(hands_over(r))
        def _():
            part[i, my_quart, :] = total.astype(jnp.bfloat16)
            m_copy(i, i - MAXB).start()

        @pl.when(jnp.logical_not(hands_over(r)))
        def _():
            part[i, my_quart, :] = live(total, r, b)
            deliver(i, r, b, s)

    def mig_a(m):
        r, b = mig_of(m)
        i = chunks + m

        @pl.when(m == 0)
        def _():
            for k in range(WPIECES):
                w_copy(k).wait_recv()

        def tile(j):
            c = pl.ds(pl.multiple_of(j * NTILE, NTILE), NTILE)
            y = jnp.dot(gath[r, b, 0], wm[:, c], preferred_element_type=jnp.float32)
            part[i, :, c] = y.astype(jnp.bfloat16)

        loop(cols // NTILE, tile)
        a_copy(i).start()

    def mig_c(m):
        r, b = mig_of(m)
        i = chunks + m
        total = reduced(i)
        m_copy(i, m).wait_recv()
        part[i, my_quart, :] = live(total + mig_in[m].astype(jnp.float32), r, b)
        deliver(i, r, b, end)

    def between(i, low, count):
        return (i >= low) & (i < low + count)

    def step(i):
        @pl.when(i < chunks)
        def _():
            stage_a(i)

        @pl.when(between(i, LAG_B, chunks))
        def _():
            stage_b(i - LAG_B)

        @pl.when(is_pre & between(i, MLAG_A, nmig))
        def _():
            mig_a(i - MLAG_A)

        @pl.when(is_pre & between(i, MLAG_A + LAG_B, nmig))
        def _():
            stage_b(chunks + i - MLAG_A - LAG_B)

        @pl.when(is_end & between(i, LAG_C, chunks))
        def _():
            stage_c(i - LAG_C)

        def pairs(cond, count, fn):
            @pl.when(cond & between(i, late, -(-count // 2)))
            def _():
                for k in range(2):
                    n = 2 * (i - late) + k

                    @pl.when(n < count)
                    def _():
                        fn(n)

        pairs(jnp.logical_not(is_end), chunks, stage_c)
        pairs(is_pre, nmig, mig_c)

    late = chunks - LATE
    loop(max(chunks + LAG_C, late + -(-chunks // 2)), step)

    def drain_send(i):
        r, b = chunk_of(i)
        for h in range(PIECES):
            for side in (1, 0):
                @pl.when(goes(h, r, side) & ((r == s) | jnp.logical_not(is_end)))
                def _():
                    g_copy(h, r, b, side).wait_send()

        a_copy(i).wait_send()
        for k in range(1, nx):
            b_copy(i, k).wait_send()

        @pl.when(hands_over(r))
        def _():
            m_copy(i, i - MAXB).wait_send()

        @pl.when(jnp.logical_not(hands_over(r) | stays(r, s)))
        def _():
            f_copy(i, r, b, s).wait_send()

    loop(chunks, drain_send)

    @pl.when(is_pre)
    def _():
        def drain_mig(m):
            r, b = mig_of(m)
            i = chunks + m
            a_copy(i).wait_send()
            for k in range(1, nx):
                b_copy(i, k).wait_send()

            @pl.when(jnp.logical_not(stays(r, end)))
            def _():
                f_copy(i, r, b, end).wait_send()

        loop(nmig, drain_mig)

    @pl.when(is_end)
    def _():
        for k in range(WPIECES):
            w_copy(k).wait_send()

    def drain_prompt(r):
        for kv in range(2):
            @pl.when(has_right & (r <= s))
            def _():
                p_copy(r, 1, kv).wait_send()

            @pl.when(has_left & (r >= s))
            def _():
                p_copy(r, 0, kv).wait_send()

    loop(nseq, drain_prompt)

    def drain_out(m):
        b = lax.div(m, per * ntp)
        j = lax.div(lax.rem(m, per * ntp), ntp)
        u = lax.rem(m, ntp)
        owner = t * per + j
        far = owner != s
        origin = jnp.where(far & (owner == 0), 1, jnp.where(far & (owner == last), last - 1, owner))

        @pl.when(jnp.logical_not((origin == s) & (u == t)))
        def _():
            row = b * BLOCK + lax.rem(u, 2) * half + lax.div(u, 2) * quart
            pltpu.make_async_remote_copy(
                src_ref=part.at[0, my_quart],
                dst_ref=out_ref.at[j, pl.ds(row, quart)],
                send_sem=f_send.at[0],
                recv_sem=f_recv.at[b, j, u],
                device_id={"seq": s, "tp": partner},
                device_id_type=MESH,
            ).wait_recv()

    loop(MAXB * per * ntp, drain_out)


def per_device(
    resp_queries, resp_keys, resp_values, prompt_keys, prompt_values, out_weight, resp_blocks
):
    nseq = lax.axis_size("seq")
    ntp = lax.axis_size("tp")
    rows, depth = resp_queries.shape
    assert rows == MAXB * BLOCK and nseq % ntp == 0 and ntp % 2 == 0 and nseq >= 4
    nx, per, chunks = ntp // 2, nseq // ntp, nseq * MAXB
    nmig = (nseq - 1) * MAXB
    every = chunks + nmig
    cols = out_weight.shape[1]
    mig = depth // PIECES
    group = depth // resp_keys.shape[1]
    assert mig % HD == 0 and group % (mig // HD) == 0
    prows, kvw = prompt_keys.shape
    quart = BLOCK // ntp
    bf = jnp.bfloat16
    dma = pltpu.SemaphoreType.DMA
    vmem = pl.BlockSpec(memory_space=pltpu.VMEM)
    out = pl.pallas_call(
        functools.partial(fused_kernel, nseq, ntp, group),
        out_shape=jax.ShapeDtypeStruct((per, rows, cols), bf),
        in_specs=[pl.BlockSpec(memory_space=pltpu.SMEM)]
        + [vmem] * 5
        + [pl.BlockSpec(memory_space=pl.ANY)],
        out_specs=vmem,
        scratch_shapes=[
            pltpu.VMEM((nseq * prows, kvw), bf),
            pltpu.VMEM((nseq * prows, kvw), bf),
            pltpu.VMEM((depth, cols), bf),
            pltpu.VMEM((mig, cols), bf),
            pltpu.VMEM((nseq, MAXB, PIECES, BLOCK, mig), bf),
            pltpu.VMEM((every, BLOCK, cols), bf),
            pltpu.VMEM((every, BLOCK // 2, cols), bf),
            pltpu.VMEM((every, max(nx - 1, 1), quart, cols), bf),
            pltpu.VMEM((nmig, quart, cols), bf),
            dma((2, nseq, 2)),
            dma((nseq, 2)),
            dma((WPIECES,)),
            dma((WPIECES,)),
            dma((WPIECES,)),
            dma((PIECES, 2, nseq, MAXB)),
            dma((PIECES, nseq, MAXB)),
            dma((every,)),
            dma((every,)),
            dma((every, max(nx - 1, 1))),
            dma((every, max(nx - 1, 1))),
            dma((every,)),
            dma((MAXB, per, ntp)),
            dma((nmig,)),
        ],
        compiler_params=pltpu.CompilerParams(
            has_side_effects=True, vmem_limit_bytes=61000 * 1024
        ),
    )(resp_blocks, resp_queries, resp_keys, resp_values, prompt_keys, prompt_values, out_weight)
    return out.transpose(1, 0, 2).reshape(rows, per * cols)


def solution(mesh):
    return jax.shard_map(
        per_device,
        mesh=mesh,
        in_specs=(
            P(("groups", "seq"), "tp"),
            P(("groups", "seq"), "tp"),
            P(("groups", "seq"), "tp"),
            P(("groups", "seq"), "tp"),
            P(("groups", "seq"), "tp"),
            P("tp", "seq"),
            P("groups"),
        ),
        out_specs=P(("groups", "seq"), "tp"),
        check_vma=False,
    )
```

```python
import functools
import jax
import jax.numpy as jnp
from jax import lax
from jax.experimental import pallas as pl
from jax.experimental.pallas import tpu as pltpu
from jax.sharding import PartitionSpec as P

HD = 128
BLOCK = 128
MAXB = 4
LOG2E = 1.4426950408889634


def scores(q, kp, kr):
    nt = (((1,), (1,)), ((), ()))
    sp = lax.dot_general(q, kp, nt, preferred_element_type=jnp.float32)
    sr = lax.dot_general(q, kr, nt, preferred_element_type=jnp.float32)
    return sp, sr


def attend(sp, sr, vp, vr, first, rows):
    c = (HD ** -0.5) * LOG2E
    qpos = lax.broadcasted_iota(jnp.int32, sr.shape, 0) % rows + first
    kpos = lax.broadcasted_iota(jnp.int32, sr.shape, 1)
    sr = jnp.where(kpos <= qpos, sr, -1e30)
    m = jnp.maximum(
        jnp.max(sp, axis=1, keepdims=True), jnp.max(sr, axis=1, keepdims=True)
    )
    ep = jnp.exp2((sp - m) * c)
    er = jnp.exp2((sr - m) * c)
    total = jnp.sum(ep, axis=1, keepdims=True) + jnp.sum(er, axis=1, keepdims=True)
    acc = jnp.dot(ep.astype(jnp.bfloat16), vp, preferred_element_type=jnp.float32)
    acc = acc + jnp.dot(er.astype(jnp.bfloat16), vr, preferred_element_type=jnp.float32)
    return (acc / total).astype(jnp.bfloat16)


MESH = pl.DeviceIdType.MESH
PIECES = 4
ORDER = (1, 2, 3, 0)
NTILE = 512
SCORES = 3 << 18
LAG_B = 1
LAG_C = 3
MLAG_A = MAXB + 1
LATE = 1


def fused_kernel(
    nseq, ntp, group,
    lens_ref, pk_ref, pv_ref, q_hbm, kr_hbm, vr_hbm, w_hbm, out_ref,
    q_ref, kr_ref, vr_ref, pk_all, pv_all, w_ref, wm, gath, part, half_in, quart_in, mig_in,
    in_sem, p_send, p_recv, w_sem, wm_send, wm_recv, g_send, g_recv,
    a_send, a_recv, b_send, b_recv, f_send, f_recv, m_recv,
):
    s = lax.axis_index("seq")
    t = lax.axis_index("tp")
    core, x = lax.rem(t, 2), lax.div(t, 2)
    partner = t + 1 - 2 * core
    nx = ntp // 2
    per = nseq // ntp
    last = nseq - 1
    chunks = nseq * MAXB
    nmig = last * MAXB
    prows = pk_ref.shape[0]
    depth, cols = w_ref.shape
    mig = wm.shape[0]
    half = BLOCK // 2
    quart = half // nx
    my_quart = pl.ds(core * half + x * quart, quart)
    kv_local = kr_ref.shape[1] // HD
    has_right, has_left = s < last, s > 0
    is_end = (s == 0) | (s == last)
    is_pre = (s == 1) | (s == last - 1)
    end = jnp.where(s < nseq // 2, 0, last)
    inward = jnp.where(s < nseq // 2, 1, -1)

    def kind(i):
        return jnp.where(i < chunks, 0, 1)

    def p_copy(r, side, kv, own=False):
        dst = (pk_all, pv_all)[kv]
        src = (pk_ref, pv_ref)[kv] if own else dst.at[pl.ds(r * prows, prows)]
        return pltpu.make_async_remote_copy(
            src_ref=src,
            dst_ref=dst.at[pl.ds(r * prows, prows)],
            send_sem=p_send.at[side, r],
            recv_sem=p_recv.at[r],
            device_id={"seq": s - 1 + 2 * side},
            device_id_type=MESH,
        )

    def p_pair(r, side):
        both_kinds = pk_all.at[pl.ds(0, 2 * prows)]
        return pltpu.make_async_remote_copy(
            src_ref=both_kinds,
            dst_ref=both_kinds,
            send_sem=p_send.at[side, r],
            recv_sem=p_recv.at[r],
            device_id={"seq": s - 1 + 2 * side},
            device_id_type=MESH,
        )

    w_local = pltpu.make_async_copy(w_hbm, w_ref, w_sem)
    w_copy = pltpu.make_async_remote_copy(
        src_ref=w_hbm.at[pl.ds(0, mig)],
        dst_ref=wm,
        send_sem=wm_send,
        recv_sem=wm_recv,
        device_id={"seq": jnp.where(is_end, s + inward, end)},
        device_id_type=MESH,
    )

    def g_copy(h, r, b, side):
        return pltpu.make_async_remote_copy(
            src_ref=gath.at[r, b, h],
            dst_ref=gath.at[r, b, h],
            send_sem=g_send.at[side, r],
            recv_sem=g_recv.at[h, r, b],
            device_id={"seq": s - 1 + 2 * side},
            device_id_type=MESH,
        )

    def a_copy(i):
        return pltpu.make_async_remote_copy(
            src_ref=part.at[i, pl.ds((1 - core) * half, half)],
            dst_ref=half_in.at[i],
            send_sem=a_send.at[kind(i)],
            recv_sem=a_recv.at[i],
            device_id={"tp": partner},
            device_id_type=MESH,
        )

    def b_copy(i, k):
        other = lax.rem(x + k, nx)
        return pltpu.make_async_remote_copy(
            src_ref=part.at[i, pl.ds(core * half + other * quart, quart)],
            dst_ref=quart_in.at[i, k - 1],
            send_sem=b_send.at[kind(i), k - 1],
            recv_sem=b_recv.at[i, k - 1],
            device_id={"tp": other * 2 + core},
            device_id_type=MESH,
        )

    def row_of(b):
        return b * BLOCK + core * half + x * quart

    def f_copy(i, r, b, owner):
        home, slab = lax.div(owner, per), lax.rem(owner, per)
        return pltpu.make_async_remote_copy(
            src_ref=part.at[i, my_quart],
            dst_ref=out_ref.at[slab, pl.ds(row_of(b), quart)],
            send_sem=f_send.at[kind(i)],
            recv_sem=f_recv.at[slab],
            device_id={"seq": r, "tp": home},
            device_id_type=MESH,
        )

    def m_copy(i, m):
        return pltpu.make_async_remote_copy(
            src_ref=part.at[i, my_quart],
            dst_ref=mig_in.at[m],
            send_sem=f_send.at[kind(i)],
            recv_sem=m_recv.at[m],
            device_id={"seq": jnp.where(is_end, s + inward, end)},
            device_id_type=MESH,
        )

    both = jnp.minimum(s, last - s)
    far_side = jnp.where(s > last - s, -1, 1)

    def chunk_of(i):
        j = jnp.maximum(i - MAXB, 0)
        twin = 2 * MAXB
        jj = jnp.maximum(j - twin * both, 0)
        near = j < twin * both
        d = jnp.where(near, lax.div(j, twin) + 1, both + 1 + lax.div(jj, MAXB))
        b = jnp.where(near, lax.div(lax.rem(j, twin), 2), lax.rem(jj, MAXB))
        side = jnp.where(near, 2 * lax.rem(j, 2) - 1, far_side)
        before = jnp.clip(lax.div(j - 2, 2), 0, MAXB)
        outer = (j >= 3) & (j < 3 + twin) & (lax.rem(j, 2) == 1)
        inner = j - before
        side = jnp.where(is_pre, jnp.where(outer, -inward, inward), side)
        d = jnp.where(is_pre, jnp.where(outer, 1, 1 + lax.div(inner, MAXB)), d)
        b = jnp.where(is_pre, jnp.where(outer, before, lax.rem(inner, MAXB)), b)
        own = i < MAXB
        return jnp.where(own, s, s + side * d), jnp.where(own, i, b)

    def mig_of(m):
        return end + inward * (1 + lax.div(m, MAXB)), lax.rem(m, MAXB)

    def loop(n, fn, start=0):
        def step(i, carry):
            fn(i)
            return carry

        lax.fori_loop(start, n, step, 0)

    def goes(h, r, side):
        if side:
            ok = has_right & (r <= s)
            return ok & (s + 1 < last) if h == 0 else ok
        ok = has_left & (r >= s)
        return ok & (s > 1) if h == 0 else ok

    def send(h, r, b):
        for side in (1, 0):
            @pl.when(goes(h, r, side))
            def _():
                g_copy(h, r, b, side).start()

    inputs = [
        pltpu.make_async_copy(src, dst, in_sem.at[k])
        for k, (src, dst) in enumerate(((q_hbm, q_ref), (kr_hbm, kr_ref), (vr_hbm, vr_ref)))
    ]
    barrier = pltpu.get_barrier_semaphore()
    peers = nseq * ntp

    def greet(k):
        other = lax.rem(s * ntp + t + k, peers)
        pl.semaphore_signal(
            barrier,
            inc=1,
            device_id={"seq": lax.div(other, ntp), "tp": lax.rem(other, ntp)},
            device_id_type=MESH,
        )

    loop(peers, greet, 1)
    for copy in inputs:
        copy.start()
    pl.semaphore_wait(barrier, peers - 1)

    for side, ok in ((0, has_left), (1, has_right)):
        @pl.when(ok)
        def _():
            p_copy(s, side, 0, own=True).start()
            p_copy(s, side, 1, own=True).start()

    @pl.when(is_end)
    def _():
        w_copy.start()

    w_local.start()

    pk_all[pl.ds(s * prows, prows), :] = pk_ref[...]
    pv_all[pl.ds(s * prows, prows), :] = pv_ref[...]

    def gather_prompt(d):
        for ok, r, side, onward in (
            (s - d >= 0, s - d, 1, has_right),
            (s + d < nseq, s + d, 0, has_left),
        ):
            @pl.when(ok)
            def _():
                p_pair(r, side).wait_recv()

                @pl.when(onward)
                def _():
                    for kv in range(2):
                        p_copy(r, side, kv).start()

    loop(nseq, gather_prompt, 1)
    for copy in inputs:
        copy.wait()

    def times(r, b, c, pieces):
        y = 0.0
        for h in pieces:
            y = y + jnp.dot(
                gath[r, b, h], w_ref[h * mig : (h + 1) * mig, c], preferred_element_type=jnp.float32
            )
        return y.astype(jnp.bfloat16)

    def project(i, r, b, full):
        for ok, pieces in ((full, range(PIECES)), (jnp.logical_not(full), range(1, PIECES))):
            @pl.when(ok)
            def _():
                def tile(j):
                    c = pl.ds(pl.multiple_of(j * NTILE, NTILE), NTILE)
                    part[i, :, c] = times(r, b, c, pieces)

                loop(cols // NTILE, tile)

        a_copy(i).start()

    def stage_a(i):
        r, b = chunk_of(i)

        @pl.when(i < MAXB)
        def _():
            first = i * BLOCK
            heads = mig // HD
            run = min(max(group // 2, 1), heads)
            while run % 2 == 0 and run * BLOCK * pk_all.shape[0] > SCORES:
                run //= 2
            runs = [h for p in ORDER for h in range(p * heads, (p + 1) * heads, run)]

            def kv_cols(h):
                return slice(h // group * HD, (h // group + 1) * HD)

            def score(h):
                q = jnp.concatenate(
                    [
                        q_ref[pl.ds(first, BLOCK), (h + g) * HD : (h + g + 1) * HD]
                        for g in range(run)
                    ],
                    axis=0,
                )
                return scores(q, pk_all[:, kv_cols(h)], kr_ref[:, kv_cols(h)])

            ready = score(runs[0])
            for n, h in enumerate(runs):
                now = ready
                if n + 1 < len(runs):
                    ready = score(runs[n + 1])
                o = attend(*now, pv_all[:, kv_cols(h)], vr_ref[:, kv_cols(h)], first, BLOCK)
                p = h // heads
                for g in range(run):
                    at = (h + g - p * heads) * HD
                    gath[s, i, p, :, at : at + HD] = o[g * BLOCK : (g + 1) * BLOCK]
                if h + run == (p + 1) * heads:
                    send(p, s, i)

        @pl.when(i >= MAXB)
        def _():
            for p in ORDER:
                @pl.when(jnp.logical_not(is_end) | (p > 0))
                def _():
                    g_copy(p, r, b, 0).wait_recv()

                send(p, r, b)

        @pl.when(i == 0)
        def _():
            w_local.wait()

        project(i, r, b, (i < MAXB) | jnp.logical_not(is_end))

    def stage_b(i):
        a_copy(i).wait_recv()
        mine = pl.ds(core * half, half)
        part[i, mine, :] = (
            part[i, mine, :].astype(jnp.float32) + half_in[i].astype(jnp.float32)
        ).astype(jnp.bfloat16)
        for k in range(1, nx):
            b_copy(i, k).start()

    def reduced(i):
        for k in range(1, nx):
            b_copy(i, k).wait_recv()
        total = part[i, my_quart, :].astype(jnp.float32)
        for k in range(1, nx):
            total = total + quart_in[i, k - 1].astype(jnp.float32)
        return total

    def live(total, r, b):
        row = lax.broadcasted_iota(jnp.int32, total.shape, 0) + row_of(b)
        return jnp.where(row < lens_ref[r] * BLOCK, total, 0.0).astype(jnp.bfloat16)

    def stays(r, owner):
        return (r == s) & (lax.div(owner, per) == t)

    def deliver(i, r, b, owner):
        here = stays(r, owner)

        @pl.when(here)
        def _():
            out_ref[lax.rem(owner, per), pl.ds(row_of(b), quart), :] = part[i, my_quart, :]

        @pl.when(jnp.logical_not(here))
        def _():
            f_copy(i, r, b, owner).start()

    def hands_over(r):
        return is_end & (r != s)

    def stage_c(i):
        r, b = chunk_of(i)
        total = reduced(i)

        @pl.when(hands_over(r))
        def _():
            part[i, my_quart, :] = total.astype(jnp.bfloat16)
            m_copy(i, i - MAXB).start()

        @pl.when(jnp.logical_not(hands_over(r)))
        def _():
            part[i, my_quart, :] = live(total, r, b)
            deliver(i, r, b, s)

    def mig_a(m):
        r, b = mig_of(m)
        i = chunks + m

        @pl.when(m == 0)
        def _():
            w_copy.wait_recv()

        def tile(j):
            c = pl.ds(pl.multiple_of(j * NTILE, NTILE), NTILE)
            y = jnp.dot(gath[r, b, 0], wm[:, c], preferred_element_type=jnp.float32)
            part[i, :, c] = y.astype(jnp.bfloat16)

        loop(cols // NTILE, tile)
        a_copy(i).start()

    def mig_c(m):
        r, b = mig_of(m)
        i = chunks + m
        total = reduced(i)
        m_copy(i, m).wait_recv()
        part[i, my_quart, :] = live(total + mig_in[m].astype(jnp.float32), r, b)
        deliver(i, r, b, end)

    def between(i, low, count):
        return (i >= low) & (i < low + count)

    def step(i):
        @pl.when(i < chunks)
        def _():
            stage_a(i)

        @pl.when(between(i, LAG_B, chunks))
        def _():
            stage_b(i - LAG_B)

        @pl.when(is_pre & between(i, MLAG_A, nmig))
        def _():
            mig_a(i - MLAG_A)

        @pl.when(is_pre & between(i, MLAG_A + LAG_B, nmig))
        def _():
            stage_b(chunks + i - MLAG_A - LAG_B)

        @pl.when(between(i, LAG_C, jnp.where(is_end, chunks, MAXB)))
        def _():
            stage_c(i - LAG_C)

        def pairs(cond, count, fn):
            @pl.when(cond & between(i, late, -(-count // 2)))
            def _():
                for k in range(2):
                    n = 2 * (i - late) + k

                    @pl.when(n < count)
                    def _():
                        fn(n)

        pairs(jnp.logical_not(is_end), chunks - MAXB, lambda n: stage_c(n + MAXB))
        pairs(is_pre, nmig, mig_c)

    late = chunks - LATE
    loop(max(chunks + LAG_C, late + -(-chunks // 2)), step)

    def drain(ref, send_sem=None, recv_sem=None):
        return pltpu.make_async_remote_copy(
            src_ref=ref,
            dst_ref=ref,
            send_sem=f_send.at[0] if send_sem is None else send_sem,
            recv_sem=f_recv.at[0] if recv_sem is None else recv_sem,
            device_id={"tp": partner},
            device_id_type=MESH,
        )

    def drain_gathered(r):
        for side, ok, whole in (
            (1, has_right & (r <= s), s + 1 < last),
            (0, has_left & (r >= s), s > 1),
        ):
            @pl.when(ok & whole)
            def _():
                drain(gath.at[r], g_send.at[side, r]).wait_send()

            @pl.when(ok & jnp.logical_not(whole))
            def _():
                drain(gath.at[r, :, pl.ds(1, PIECES - 1)], g_send.at[side, r]).wait_send()

            @pl.when(ok)
            def _():
                p_pair(r, side).wait_send()

    loop(nseq, drain_gathered)

    for n, low, count, cond, owner in (
        (0, 0, chunks, None, s),
        (1, chunks, nmig, is_pre, end),
    ):
        local = lax.div(owner, per) == t
        yes = s >= 0 if cond is None else cond

        @pl.when(yes)
        def _():
            drain(half_in.at[pl.ds(low, count)], a_send.at[n]).wait_send()
            for k in range(1, nx):
                drain(quart_in.at[pl.ds(low, count), k - 1], b_send.at[n, k - 1]).wait_send()

        for here in (True, False):
            @pl.when(yes & (local if here else jnp.logical_not(local)))
            def _():
                sent = count - MAXB if here else count
                drain(part.at[pl.ds(low, sent), pl.ds(0, quart)], f_send.at[n]).wait_send()

    @pl.when(is_end)
    def _():
        w_copy.wait_send()

    for j in range(per):
        owner = t * per + j
        far = owner != s
        origin = jnp.where(far & (owner == 0), 1, jnp.where(far & (owner == last), last - 1, owner))
        rows = out_ref.shape[1]
        for here in (True, False):
            @pl.when(origin == s if here else origin != s)
            def _():
                count = rows - MAXB * quart if here else rows
                drain(out_ref.at[j, pl.ds(0, count)], recv_sem=f_recv.at[j]).wait_recv()


def per_device(
    resp_queries, resp_keys, resp_values, prompt_keys, prompt_values, out_weight, resp_blocks
):
    nseq = lax.axis_size("seq")
    ntp = lax.axis_size("tp")
    rows, depth = resp_queries.shape
    assert rows == MAXB * BLOCK and nseq % ntp == 0 and ntp % 2 == 0 and nseq >= 4
    nx, per, chunks = ntp // 2, nseq // ntp, nseq * MAXB
    nmig = (nseq - 1) * MAXB
    every = chunks + nmig
    cols = out_weight.shape[1]
    mig = depth // PIECES
    group = depth // resp_keys.shape[1]
    assert mig % HD == 0 and group % (mig // HD) == 0
    prows, kvw = prompt_keys.shape
    quart = BLOCK // ntp
    bf = jnp.bfloat16
    dma = pltpu.SemaphoreType.DMA
    vmem = pl.BlockSpec(memory_space=pltpu.VMEM)
    out = pl.pallas_call(
        functools.partial(fused_kernel, nseq, ntp, group),
        out_shape=jax.ShapeDtypeStruct((per, rows, cols), bf),
        in_specs=[pl.BlockSpec(memory_space=pltpu.SMEM)]
        + [vmem] * 2
        + [pl.BlockSpec(memory_space=pl.ANY)] * 4,
        out_specs=vmem,
        scratch_shapes=[
            pltpu.VMEM(resp_queries.shape, bf),
            pltpu.VMEM(resp_keys.shape, bf),
            pltpu.VMEM(resp_values.shape, bf),
            pltpu.VMEM((nseq * prows, kvw), bf),
            pltpu.VMEM((nseq * prows, kvw), bf),
            pltpu.VMEM((depth, cols), bf),
            pltpu.VMEM((mig, cols), bf),
            pltpu.VMEM((nseq, MAXB, PIECES, BLOCK, mig), bf),
            pltpu.VMEM((every, BLOCK, cols), bf),
            pltpu.VMEM((every, BLOCK // 2, cols), bf),
            pltpu.VMEM((every, max(nx - 1, 1), quart, cols), bf),
            pltpu.VMEM((nmig, quart, cols), bf),
            dma((3,)),
            dma((2, nseq)),
            dma((nseq,)),
            dma,
            dma,
            dma,
            dma((2, nseq)),
            dma((PIECES, nseq, MAXB)),
            dma((2,)),
            dma((every,)),
            dma((2, max(nx - 1, 1))),
            dma((every, max(nx - 1, 1))),
            dma((2,)),
            dma((per,)),
            dma((nmig,)),
        ],
        compiler_params=pltpu.CompilerParams(
            has_side_effects=True, collective_id=0, vmem_limit_bytes=61000 * 1024
        ),
    )(resp_blocks, prompt_keys, prompt_values, resp_queries, resp_keys, resp_values, out_weight)
    return out.transpose(1, 0, 2).reshape(rows, per * cols)


def solution(mesh):
    return jax.shard_map(
        per_device,
        mesh=mesh,
        in_specs=(
            P(("groups", "seq"), "tp"),
            P(("groups", "seq"), "tp"),
            P(("groups", "seq"), "tp"),
            P(("groups", "seq"), "tp"),
            P(("groups", "seq"), "tp"),
            P("tp", "seq"),
            P("groups"),
        ),
        out_specs=P(("groups", "seq"), "tp"),
        check_vma=False,
    )
```

```python
import functools
import jax
import jax.numpy as jnp
from jax import lax
from jax.experimental import pallas as pl
from jax.experimental.pallas import tpu as pltpu
from jax.sharding import PartitionSpec as P

HD = 128
BLOCK = 128
MAXB = 4
LOG2E = 1.4426950408889634


def scores(q, kp, kr):
    nt = (((1,), (1,)), ((), ()))
    sp = lax.dot_general(q, kp, nt, preferred_element_type=jnp.float32)
    sr = lax.dot_general(q, kr, nt, preferred_element_type=jnp.float32)
    return sp, sr


def attend(sp, sr, vp, vr, first, rows):
    c = (HD ** -0.5) * LOG2E
    qpos = lax.broadcasted_iota(jnp.int32, sr.shape, 0) % rows + first
    kpos = lax.broadcasted_iota(jnp.int32, sr.shape, 1)
    sr = jnp.where(kpos <= qpos, sr, -1e30)
    m = jnp.maximum(
        jnp.max(sp, axis=1, keepdims=True), jnp.max(sr, axis=1, keepdims=True)
    )
    ep = jnp.exp2((sp - m) * c)
    er = jnp.exp2((sr - m) * c)
    total = jnp.sum(ep, axis=1, keepdims=True) + jnp.sum(er, axis=1, keepdims=True)
    acc = jnp.dot(ep.astype(jnp.bfloat16), vp, preferred_element_type=jnp.float32)
    acc = acc + jnp.dot(er.astype(jnp.bfloat16), vr, preferred_element_type=jnp.float32)
    return (acc / total).astype(jnp.bfloat16)


MESH = pl.DeviceIdType.MESH
PIECES = 4
ORDER = (1, 2, 3, 0)
NTILE = 512
SCORES = 3 << 18
LAG_B = 1
LAG_C = 3
MLAG_A = MAXB + 1
LATE = 1


def fused_kernel(
    nseq, ntp, group,
    lens_ref, pk_ref, pv_ref, q_hbm, kr_hbm, vr_hbm, w_hbm, out_ref,
    q_ref, kr_ref, vr_ref, pk_all, pv_all, w_ref, wm, gath, part, half_in, quart_in, mig_in,
    in_sem, p_send, p_recv, w_sem, wm_send, wm_recv, g_send, g_recv,
    a_send, a_recv, b_send, b_recv, f_send, f_recv, m_recv,
):
    s = lax.axis_index("seq")
    t = lax.axis_index("tp")
    core, x = lax.rem(t, 2), lax.div(t, 2)
    partner = t + 1 - 2 * core
    nx = ntp // 2
    per = nseq // ntp
    last = nseq - 1
    chunks = nseq * MAXB
    nmig = last * MAXB
    prows = pk_ref.shape[0]
    depth, cols = w_ref.shape
    mig = wm.shape[0]
    half = BLOCK // 2
    quart = half // nx
    my_quart = pl.ds(core * half + x * quart, quart)
    kv_local = kr_ref.shape[1] // HD
    has_right, has_left = s < last, s > 0
    is_end = (s == 0) | (s == last)
    is_pre = (s == 1) | (s == last - 1)
    end = jnp.where(s < nseq // 2, 0, last)
    inward = jnp.where(s < nseq // 2, 1, -1)

    def kind(i):
        return jnp.where(i < chunks, 0, 1)

    def p_copy(r, side, kv, own=False):
        dst = (pk_all, pv_all)[kv]
        src = (pk_ref, pv_ref)[kv] if own else dst.at[pl.ds(r * prows, prows)]
        return pltpu.make_async_remote_copy(
            src_ref=src,
            dst_ref=dst.at[pl.ds(r * prows, prows)],
            send_sem=p_send.at[side, r],
            recv_sem=p_recv.at[r, kv],
            device_id={"seq": s - 1 + 2 * side},
            device_id_type=MESH,
        )

    def p_pair(r, side):
        both_kinds = pk_all.at[pl.ds(0, 2 * prows)]
        return pltpu.make_async_remote_copy(
            src_ref=both_kinds,
            dst_ref=both_kinds,
            send_sem=p_send.at[side, r],
            recv_sem=p_recv.at[r, 0],
            device_id={"seq": s - 1 + 2 * side},
            device_id_type=MESH,
        )

    w_local = pltpu.make_async_copy(w_hbm, w_ref, w_sem)
    w_copy = pltpu.make_async_remote_copy(
        src_ref=w_ref.at[pl.ds(0, mig)],
        dst_ref=wm,
        send_sem=wm_send,
        recv_sem=wm_recv,
        device_id={"seq": jnp.where(is_end, s + inward, end)},
        device_id_type=MESH,
    )

    def g_copy(h, r, b, side):
        return pltpu.make_async_remote_copy(
            src_ref=gath.at[r, b, h],
            dst_ref=gath.at[r, b, h],
            send_sem=g_send.at[side, r],
            recv_sem=g_recv.at[h, r, b],
            device_id={"seq": s - 1 + 2 * side},
            device_id_type=MESH,
        )

    def a_copy(i):
        return pltpu.make_async_remote_copy(
            src_ref=part.at[i, pl.ds((1 - core) * half, half)],
            dst_ref=half_in.at[i],
            send_sem=a_send.at[kind(i)],
            recv_sem=a_recv.at[i],
            device_id={"tp": partner},
            device_id_type=MESH,
        )

    def b_copy(i, k):
        other = lax.rem(x + k, nx)
        return pltpu.make_async_remote_copy(
            src_ref=part.at[i, pl.ds(core * half + other * quart, quart)],
            dst_ref=quart_in.at[i, k - 1],
            send_sem=b_send.at[kind(i), k - 1],
            recv_sem=b_recv.at[i, k - 1],
            device_id={"tp": other * 2 + core},
            device_id_type=MESH,
        )

    def row_of(b):
        return b * BLOCK + core * half + x * quart

    def f_copy(i, r, b, owner):
        home, slab = lax.div(owner, per), lax.rem(owner, per)
        return pltpu.make_async_remote_copy(
            src_ref=part.at[i, my_quart],
            dst_ref=out_ref.at[slab, pl.ds(row_of(b), quart)],
            send_sem=f_send.at[kind(i)],
            recv_sem=f_recv.at[slab],
            device_id={"seq": r, "tp": home},
            device_id_type=MESH,
        )

    def m_copy(i, m):
        return pltpu.make_async_remote_copy(
            src_ref=part.at[i, my_quart],
            dst_ref=mig_in.at[m],
            send_sem=f_send.at[kind(i)],
            recv_sem=m_recv.at[m],
            device_id={"seq": jnp.where(is_end, s + inward, end)},
            device_id_type=MESH,
        )

    both = jnp.minimum(s, last - s)
    far_side = jnp.where(s > last - s, -1, 1)

    def chunk_of(i):
        j = jnp.maximum(i - MAXB, 0)
        twin = 2 * MAXB
        jj = jnp.maximum(j - twin * both, 0)
        near = j < twin * both
        d = jnp.where(near, lax.div(j, twin) + 1, both + 1 + lax.div(jj, MAXB))
        b = jnp.where(near, lax.div(lax.rem(j, twin), 2), lax.rem(jj, MAXB))
        side = jnp.where(near, 2 * lax.rem(j, 2) - 1, far_side)
        before = jnp.clip(lax.div(j - 2, 2), 0, MAXB)
        outer = (j >= 3) & (j < 3 + twin) & (lax.rem(j, 2) == 1)
        inner = j - before
        side = jnp.where(is_pre, jnp.where(outer, -inward, inward), side)
        d = jnp.where(is_pre, jnp.where(outer, 1, 1 + lax.div(inner, MAXB)), d)
        b = jnp.where(is_pre, jnp.where(outer, before, lax.rem(inner, MAXB)), b)
        own = i < MAXB
        return jnp.where(own, s, s + side * d), jnp.where(own, i, b)

    def mig_of(m):
        return end + inward * (1 + lax.div(m, MAXB)), lax.rem(m, MAXB)

    def loop(n, fn, start=0):
        def step(i, carry):
            fn(i)
            return carry

        lax.fori_loop(start, n, step, 0)

    def goes(h, r, side):
        if side:
            ok = has_right & (r <= s)
            return ok & (s + 1 < last) if h == 0 else ok
        ok = has_left & (r >= s)
        return ok & (s > 1) if h == 0 else ok

    def send(h, r, b):
        for side in (1, 0):
            @pl.when(goes(h, r, side))
            def _():
                g_copy(h, r, b, side).start()

    inputs = [
        pltpu.make_async_copy(src, dst, in_sem.at[k])
        for k, (src, dst) in enumerate(((q_hbm, q_ref), (kr_hbm, kr_ref), (vr_hbm, vr_ref)))
    ]
    barrier = pltpu.get_barrier_semaphore()
    peers = nseq * ntp

    def greet(k):
        other = lax.rem(s * ntp + t + k, peers)
        pl.semaphore_signal(
            barrier,
            inc=1,
            device_id={"seq": lax.div(other, ntp), "tp": lax.rem(other, ntp)},
            device_id_type=MESH,
        )

    loop(peers, greet, 1)
    w_local.start()
    for copy in inputs:
        copy.start()
    pl.semaphore_wait(barrier, peers - 1)

    for side, ok in ((0, has_left), (1, has_right)):
        @pl.when(ok)
        def _():
            p_copy(s, side, 0, own=True).start()
            p_copy(s, side, 1, own=True).start()

    w_local.wait()

    @pl.when(is_end)
    def _():
        w_copy.start()


    pk_all[pl.ds(s * prows, prows), :] = pk_ref[...]
    pv_all[pl.ds(s * prows, prows), :] = pv_ref[...]

    def gather_prompt(d):
        for ok, r, side, onward in (
            (s - d >= 0, s - d, 1, has_right),
            (s + d < nseq, s + d, 0, has_left),
        ):
            @pl.when(ok)
            def _():
                for kv in range(2):
                    p_copy(r, side, kv).wait_recv()

                    @pl.when(onward)
                    def _():
                        p_copy(r, side, kv).start()

    loop(nseq, gather_prompt, 1)
    for copy in inputs:
        copy.wait()

    def times(r, b, c, pieces):
        y = 0.0
        for h in pieces:
            y = y + jnp.dot(
                gath[r, b, h], w_ref[h * mig : (h + 1) * mig, c], preferred_element_type=jnp.float32
            )
        return y.astype(jnp.bfloat16)

    def project(i, r, b, full):
        for ok, pieces in ((full, range(PIECES)), (jnp.logical_not(full), range(1, PIECES))):
            @pl.when(ok)
            def _():
                def tile(j):
                    c = pl.ds(pl.multiple_of(j * NTILE, NTILE), NTILE)
                    part[i, :, c] = times(r, b, c, pieces)

                loop(cols // NTILE, tile)

        a_copy(i).start()

    def stage_a(i):
        r, b = chunk_of(i)

        @pl.when(i < MAXB)
        def _():
            first = i * BLOCK
            heads = mig // HD
            run = min(max(group // 2, 1), heads)
            while run % 2 == 0 and run * BLOCK * pk_all.shape[0] > SCORES:
                run //= 2
            runs = [h for p in ORDER for h in range(p * heads, (p + 1) * heads, run)]

            def kv_cols(h):
                return slice(h // group * HD, (h // group + 1) * HD)

            def score(h):
                q = jnp.concatenate(
                    [
                        q_ref[pl.ds(first, BLOCK), (h + g) * HD : (h + g + 1) * HD]
                        for g in range(run)
                    ],
                    axis=0,
                )
                return scores(q, pk_all[:, kv_cols(h)], kr_ref[:, kv_cols(h)])

            ready = score(runs[0])
            for n, h in enumerate(runs):
                now = ready
                if n + 1 < len(runs):
                    ready = score(runs[n + 1])
                o = attend(*now, pv_all[:, kv_cols(h)], vr_ref[:, kv_cols(h)], first, BLOCK)
                p = h // heads
                for g in range(run):
                    at = (h + g - p * heads) * HD
                    gath[s, i, p, :, at : at + HD] = o[g * BLOCK : (g + 1) * BLOCK]
                if h + run == (p + 1) * heads:
                    send(p, s, i)

        @pl.when(i >= MAXB)
        def _():
            for p in ORDER:
                @pl.when(jnp.logical_not(is_end) | (p > 0))
                def _():
                    g_copy(p, r, b, 0).wait_recv()

                send(p, r, b)

        project(i, r, b, (i < MAXB) | jnp.logical_not(is_end))

    def stage_b(i):
        a_copy(i).wait_recv()
        mine = pl.ds(core * half, half)
        part[i, mine, :] = (
            part[i, mine, :].astype(jnp.float32) + half_in[i].astype(jnp.float32)
        ).astype(jnp.bfloat16)
        for k in range(1, nx):
            b_copy(i, k).start()

    def reduced(i):
        for k in range(1, nx):
            b_copy(i, k).wait_recv()
        total = part[i, my_quart, :].astype(jnp.float32)
        for k in range(1, nx):
            total = total + quart_in[i, k - 1].astype(jnp.float32)
        return total

    def live(total, r, b):
        row = lax.broadcasted_iota(jnp.int32, total.shape, 0) + row_of(b)
        return jnp.where(row < lens_ref[r] * BLOCK, total, 0.0).astype(jnp.bfloat16)

    def stays(r, owner):
        return (r == s) & (lax.div(owner, per) == t)

    def deliver(i, r, b, owner):
        here = stays(r, owner)

        @pl.when(here)
        def _():
            out_ref[lax.rem(owner, per), pl.ds(row_of(b), quart), :] = part[i, my_quart, :]

        @pl.when(jnp.logical_not(here))
        def _():
            f_copy(i, r, b, owner).start()

    def hands_over(r):
        return is_end & (r != s)

    def stage_c(i):
        r, b = chunk_of(i)
        total = reduced(i)

        @pl.when(hands_over(r))
        def _():
            part[i, my_quart, :] = total.astype(jnp.bfloat16)
            m_copy(i, i - MAXB).start()

        @pl.when(jnp.logical_not(hands_over(r)))
        def _():
            part[i, my_quart, :] = live(total, r, b)
            deliver(i, r, b, s)

    def mig_a(m):
        r, b = mig_of(m)
        i = chunks + m

        @pl.when(m == 0)
        def _():
            w_copy.wait_recv()

        def tile(j):
            c = pl.ds(pl.multiple_of(j * NTILE, NTILE), NTILE)
            y = jnp.dot(gath[r, b, 0], wm[:, c], preferred_element_type=jnp.float32)
            part[i, :, c] = y.astype(jnp.bfloat16)

        loop(cols // NTILE, tile)
        a_copy(i).start()

    def mig_c(m):
        r, b = mig_of(m)
        i = chunks + m
        total = reduced(i)
        m_copy(i, m).wait_recv()
        part[i, my_quart, :] = live(total + mig_in[m].astype(jnp.float32), r, b)
        deliver(i, r, b, end)

    def between(i, low, count):
        return (i >= low) & (i < low + count)

    def step(i):
        @pl.when(i < chunks)
        def _():
            stage_a(i)

        @pl.when(between(i, LAG_B, chunks))
        def _():
            stage_b(i - LAG_B)

        @pl.when(is_pre & between(i, MLAG_A, nmig))
        def _():
            mig_a(i - MLAG_A)

        @pl.when(is_pre & between(i, MLAG_A + LAG_B, nmig))
        def _():
            stage_b(chunks + i - MLAG_A - LAG_B)

        @pl.when(between(i, LAG_C, jnp.where(is_end, chunks, MAXB)))
        def _():
            stage_c(i - LAG_C)

        def pairs(cond, count, fn):
            @pl.when(cond & between(i, late, -(-count // 2)))
            def _():
                for k in range(2):
                    n = 2 * (i - late) + k

                    @pl.when(n < count)
                    def _():
                        fn(n)

        pairs(jnp.logical_not(is_end), chunks - MAXB, lambda n: stage_c(n + MAXB))
        pairs(is_pre, nmig, mig_c)

    late = chunks - LATE
    loop(max(chunks + LAG_C, late + -(-chunks // 2)), step)

    def drain(ref, send_sem=None, recv_sem=None):
        return pltpu.make_async_remote_copy(
            src_ref=ref,
            dst_ref=ref,
            send_sem=f_send.at[0] if send_sem is None else send_sem,
            recv_sem=f_recv.at[0] if recv_sem is None else recv_sem,
            device_id={"tp": partner},
            device_id_type=MESH,
        )

    def drain_gathered(r):
        for side, ok, whole in (
            (1, has_right & (r <= s), s + 1 < last),
            (0, has_left & (r >= s), s > 1),
        ):
            @pl.when(ok & whole)
            def _():
                drain(gath.at[r], g_send.at[side, r]).wait_send()

            @pl.when(ok & jnp.logical_not(whole))
            def _():
                drain(gath.at[r, :, pl.ds(1, PIECES - 1)], g_send.at[side, r]).wait_send()

            @pl.when(ok)
            def _():
                p_pair(r, side).wait_send()

    loop(nseq, drain_gathered)

    for n, low, count, cond, owner in (
        (0, 0, chunks, None, s),
        (1, chunks, nmig, is_pre, end),
    ):
        local = lax.div(owner, per) == t
        yes = s >= 0 if cond is None else cond

        @pl.when(yes)
        def _():
            drain(half_in.at[pl.ds(low, count)], a_send.at[n]).wait_send()
            for k in range(1, nx):
                drain(quart_in.at[pl.ds(low, count), k - 1], b_send.at[n, k - 1]).wait_send()

        for here in (True, False):
            @pl.when(yes & (local if here else jnp.logical_not(local)))
            def _():
                sent = count - MAXB if here else count
                drain(part.at[pl.ds(low, sent), pl.ds(0, quart)], f_send.at[n]).wait_send()

    @pl.when(is_end)
    def _():
        w_copy.wait_send()

    for j in range(per):
        owner = t * per + j
        far = owner != s
        origin = jnp.where(far & (owner == 0), 1, jnp.where(far & (owner == last), last - 1, owner))
        rows = out_ref.shape[1]
        for here in (True, False):
            @pl.when(origin == s if here else origin != s)
            def _():
                count = rows - MAXB * quart if here else rows
                drain(out_ref.at[j, pl.ds(0, count)], recv_sem=f_recv.at[j]).wait_recv()


def place_kernel(steps, src, dst, held, in_sem, out_sem):
    per, rows, cols = src.shape
    tall = rows // steps

    def pair(j, k):
        at = pl.ds(k * tall, tall)
        there = dst.at[at, pl.ds(j * cols, cols)]
        return (
            pltpu.make_async_copy(src.at[j, at], held.at[j, at], in_sem.at[j, k]),
            pltpu.make_async_copy(held.at[j, at], there, out_sem.at[j, k]),
        )

    every = [pair(j, k) for j in range(per) for k in range(steps)]
    for first, _ in every:
        first.start()
    for first, second in every:
        first.wait()
        second.start()
    for _, second in every:
        second.wait()


def per_device(
    resp_queries, resp_keys, resp_values, prompt_keys, prompt_values, out_weight, resp_blocks
):
    nseq = lax.axis_size("seq")
    ntp = lax.axis_size("tp")
    rows, depth = resp_queries.shape
    assert rows == MAXB * BLOCK and nseq % ntp == 0 and ntp % 2 == 0 and nseq >= 4
    nx, per, chunks = ntp // 2, nseq // ntp, nseq * MAXB
    nmig = (nseq - 1) * MAXB
    every = chunks + nmig
    cols = out_weight.shape[1]
    mig = depth // PIECES
    group = depth // resp_keys.shape[1]
    assert mig % HD == 0 and group % (mig // HD) == 0
    prows, kvw = prompt_keys.shape
    quart = BLOCK // ntp
    bf = jnp.bfloat16
    dma = pltpu.SemaphoreType.DMA
    vmem = pl.BlockSpec(memory_space=pltpu.VMEM)
    out = pl.pallas_call(
        functools.partial(fused_kernel, nseq, ntp, group),
        out_shape=jax.ShapeDtypeStruct((per, rows, cols), bf),
        in_specs=[pl.BlockSpec(memory_space=pltpu.SMEM)]
        + [vmem] * 2
        + [pl.BlockSpec(memory_space=pl.ANY)] * 4,
        out_specs=vmem,
        scratch_shapes=[
            pltpu.VMEM(resp_queries.shape, bf),
            pltpu.VMEM(resp_keys.shape, bf),
            pltpu.VMEM(resp_values.shape, bf),
            pltpu.VMEM((nseq * prows, kvw), bf),
            pltpu.VMEM((nseq * prows, kvw), bf),
            pltpu.VMEM((depth, cols), bf),
            pltpu.VMEM((mig, cols), bf),
            pltpu.VMEM((nseq, MAXB, PIECES, BLOCK, mig), bf),
            pltpu.VMEM((every, BLOCK, cols), bf),
            pltpu.VMEM((every, BLOCK // 2, cols), bf),
            pltpu.VMEM((every, max(nx - 1, 1), quart, cols), bf),
            pltpu.VMEM((nmig, quart, cols), bf),
            dma((3,)),
            dma((2, nseq)),
            dma((nseq, 2)),
            dma,
            dma,
            dma,
            dma((2, nseq)),
            dma((PIECES, nseq, MAXB)),
            dma((2,)),
            dma((every,)),
            dma((2, max(nx - 1, 1))),
            dma((every, max(nx - 1, 1))),
            dma((2,)),
            dma((per,)),
            dma((nmig,)),
        ],
        compiler_params=pltpu.CompilerParams(
            has_side_effects=True, collective_id=0, vmem_limit_bytes=61000 * 1024
        ),
    )(resp_blocks, prompt_keys, prompt_values, resp_queries, resp_keys, resp_values, out_weight)
    steps = 8
    return pl.pallas_call(
        functools.partial(place_kernel, steps),
        out_shape=jax.ShapeDtypeStruct((rows, per * cols), bf),
        in_specs=[pl.BlockSpec(memory_space=pl.ANY)],
        out_specs=pl.BlockSpec(memory_space=pl.ANY),
        scratch_shapes=[pltpu.VMEM((per, rows, cols), bf), dma((per, steps)), dma((per, steps))],
    )(out)


def solution(mesh):
    return jax.shard_map(
        per_device,
        mesh=mesh,
        in_specs=(
            P(("groups", "seq"), "tp"),
            P(("groups", "seq"), "tp"),
            P(("groups", "seq"), "tp"),
            P(("groups", "seq"), "tp"),
            P(("groups", "seq"), "tp"),
            P("tp", "seq"),
            P("groups"),
        ),
        out_specs=P(("groups", "seq"), "tp"),
        check_vma=False,
    )
```
